32 devices in a mesh: section: 4 (over y, x), seq: 8 (over z, core).
Axes of the slice: x: 2, y: 2, z: 4, core: 2. Of those that a mesh axis runs over, the one named last changes fastest.
Arguments:
- queries: bfloat16 [4, 1024, 4096], P('section', 'seq'), may hold values from -500 to 500
- keys: bfloat16 [4, 1024, 512], P('section', 'seq'), may hold values from -6 to 6
- values: bfloat16 [4, 1024, 512], P('section', 'seq'), may hold values from -6 to 6
- out_grad: bfloat16 [4, 1024, 4096], P('section', 'seq'), may hold values from -6 to 6
- documents: int32 [4, 1024], P('section'), may hold values from 0 to 3, never falling along the last dimension, each value on 1 to 512 neighbouring positions
- query_weight: bfloat16 [4, 4096, 4096], P('section', 'seq'), may hold values from -0.09375 to 0.09375
- key_weight: bfloat16 [4, 512, 4096], P('section'), may hold values from -0.1875 to 0.1875
- value_weight: bfloat16 [4, 512, 4096], P('section'), may hold values from -0.1875 to 0.1875
Outputs:
- upstream: bfloat16 [4, 1024, 4096], P('section', 'seq')
The draws below stay inside these ranges and needn't reach their ends.
Inputs may be any that keep to these rules, and one draw needn't show every extreme that they name: `documents`: each section's document ids never fall along its tokens.
All inputs are finite; a program needn't handle non-finite values.
Results may differ from the reference program's by a relative error of at most 0.0058.
Values may be sent and summed in bfloat16 or wider, within the bound.
No kernel may reach another device: no remote copies, remote signals or barrier semaphores. Data moves between devices by JAX's collectives and lax.ppermute only.
A program may use at most 192 MiB of HBM per device.

```python
import math
import jax
import jax.numpy as jnp
import numpy as np
from jax import lax

D = 4096
H = 32
KV = 4
HD = 128
SECTIONS = 4
TOKENS = 1024
N_SEQ = 8


def query_key_pair(key):
    base = jax.random.fold_in(key, 11)
    key_q, key_k = jax.random.split(base, 2)
    queries = jax.random.normal(key_q, (SECTIONS, TOKENS, H * HD), jnp.float32)
    keys = jax.random.normal(key_k, (SECTIONS, TOKENS, KV * HD), jnp.float32)
    keys = jnp.clip(keys, -6.0, 6.0)
    return (queries, keys)


def draw_queries(key, part):
    return query_key_pair(key)[0].astype(jnp.bfloat16)


def draw_keys(key, part):
    return query_key_pair(key)[1].astype(jnp.bfloat16)


def shard_levels(rng, shape, shards, least, top_value):
    def one(axis_at, parts):
        draws = jax.random.uniform(jax.random.fold_in(jax.random.fold_in(rng, 6), axis_at), (parts,), jnp.float32, least / len(shards), top_value / len(shards))
        return jnp.repeat(jnp.exp(draws), shape[axis_at] // parts).reshape((-1,) + (1,) * (len(shape) - axis_at - 1))

    loudness = one(*shards[0])
    for cut in shards[1:]:
        loudness = loudness * one(*cut)
    return loudness


def split_up(amount, total, most, slope):
    weights = [(1 << 20) // math.isqrt(rank ** slope) + 1 for rank in range(2, amount + 1)]
    rest, counts = total - most - (amount - 1), [1] * (amount - 1)
    while rest > 0:
        movable = [i for i in range(amount - 1) if counts[i] < most]
        pool, remaining = sum([weights[i] for i in movable]), rest
        for i in movable:
            extra = min(most - counts[i], max(1, remaining * weights[i] // pool), rest)
            counts[i] = counts[i] + extra
            rest = rest - extra
    return np.array([most] + counts)


def ragged(own_key, amount, total, bound, slope):
    if amount == 2:
        one = jax.random.randint(own_key, (), max(1, total - bound), min(bound, total - 1) + 1)
        return jnp.stack([one, total - one])
    tallies = jnp.asarray(split_up(amount, total, bound, slope), jnp.int32)
    twos = (amount - 1) // 2
    donor, taker = tallies[1:1 + 2 * twos:2], tallies[2:2 + 2 * twos:2]
    slack = jnp.minimum(donor - 1, bound - taker)
    passed = jax.random.randint(jax.random.fold_in(own_key, 1), (twos,), 0, 1 << 20) % (slack + 1)
    tallies = tallies.at[1:1 + 2 * twos:2].set(donor - passed).at[2:2 + 2 * twos:2].set(taker + passed)
    return tallies[jax.random.permutation(jax.random.fold_in(own_key, 2), amount)]


def normal_values(key, dims, deviation, reach, cuts=(), kind=jnp.bfloat16):
    loudness = shard_levels(key, dims, cuts, -0.22, 0.18) if cuts else 1.0
    array = jax.random.normal(key, dims, jnp.float32) * deviation * loudness
    return jnp.minimum(jnp.maximum(array, -reach), reach).astype(kind)


def setup_inputs(seed: int = 0) -> dict:
    streams_of = jax.random.split(jax.random.key(seed), 9)
    return {
        "queries": draw_queries(jax.random.fold_in(streams_of[8], 71), 0),
        "keys": draw_keys(jax.random.fold_in(streams_of[8], 71), 0),
        "values": normal_values(streams_of[2], (SECTIONS, TOKENS, KV * HD), 1.0, 6.0, ((0, 4), (1, 8))),
        "out_grad": normal_values(streams_of[3], (SECTIONS, TOKENS, H * HD), 1.0, 6.0, ((0, 4), (1, 8))),
        "documents": jax.vmap(lambda own: jnp.searchsorted(jnp.cumsum(ragged(own, 4, TOKENS, TOKENS // 2, 0)), jnp.arange(TOKENS), side="right"))(jax.random.split(streams_of[4], SECTIONS)).reshape((SECTIONS, TOKENS)).astype(jnp.int32),
        "query_weight": normal_values(streams_of[5], (SECTIONS, H * HD, D), (H * HD) ** -0.5, 0.09375, ((0, 4), (1, 8))),
        "key_weight": normal_values(streams_of[6], (SECTIONS, KV * HD, D), (N_SEQ * HD) ** -0.5, 0.1875, ((0, 4),)),
        "value_weight": normal_values(streams_of[7], (SECTIONS, KV * HD, D), (N_SEQ * HD) ** -0.5, 0.1875, ((0, 4),)),
    }


def slot_grads(index, q_all, k_all, v_all, o_all, ids):
    per = H // N_SEQ
    total = q_all.shape[0]
    kvh = index * KV // N_SEQ
    scale = 1.0 / math.sqrt(HD)
    q_blk = lax.dynamic_slice_in_dim(q_all, index * per * HD, per * HD, 1).reshape(total, per, HD).astype(jnp.float32)
    o_blk = lax.dynamic_slice_in_dim(o_all, index * per * HD, per * HD, 1).reshape(total, per, HD).astype(jnp.float32)
    k_head = lax.dynamic_slice_in_dim(k_all, kvh * HD, HD, 1).astype(jnp.float32)
    v_head = lax.dynamic_slice_in_dim(v_all, kvh * HD, HD, 1).astype(jnp.float32)
    rows = lax.iota(jnp.int32, total)
    allowed = (rows[None, :] <= rows[:, None]) & (ids[None, :] == ids[:, None])
    scores = jnp.einsum('bhd,td->hbt', q_blk, k_head) * scale
    scores = jnp.where(allowed[None], scores, -jnp.inf)
    top = lax.optimization_barrier(jnp.max(scores, axis=-1, keepdims=True))
    expo = jnp.exp(scores - top)
    prob = expo / lax.optimization_barrier(jnp.sum(expo, axis=-1, keepdims=True))
    prob_low = prob.astype(jnp.bfloat16)
    dprob = jnp.einsum('bhd,td->hbt', o_blk, v_head)
    delta = lax.optimization_barrier(jnp.sum(prob * dprob, axis=-1, keepdims=True))
    dscore = (prob * (dprob - delta) * scale).astype(jnp.bfloat16).astype(jnp.float32)
    dquery = jnp.einsum('hbt,td->bhd', dscore, k_head).astype(jnp.bfloat16).reshape(total, per * HD)
    dkey = jnp.einsum('hbt,bhd->td', dscore, q_blk).astype(jnp.bfloat16)
    dvalue = jnp.einsum('hbt,bhd->td', prob_low.astype(jnp.float32), o_blk).astype(jnp.bfloat16)
    return (dquery, dkey, dvalue)

def reference(queries, keys, values, out_grad, documents, query_weight, key_weight, value_weight):
    reps = N_SEQ // KV
    grads = []
    for section in range(SECTIONS):

        def one_slot(index):
            return slot_grads(index, queries[section], keys[section], values[section], out_grad[section], documents[section])
        dq_s, dk_s, dv_s = lax.map(one_slot, jnp.arange(N_SEQ, dtype=jnp.int32))
        total = queries.shape[1]
        dquery = jnp.transpose(dq_s, (1, 0, 2)).reshape(total, H * HD)
        dkey = jnp.transpose(dk_s, (1, 0, 2)).reshape(total, N_SEQ * HD)
        dvalue = jnp.transpose(dv_s, (1, 0, 2)).reshape(total, N_SEQ * HD)
        wk_rep = jnp.repeat(key_weight[section].reshape(KV, HD, D), reps, axis=0).reshape(N_SEQ * HD, D)
        wv_rep = jnp.repeat(value_weight[section].reshape(KV, HD, D), reps, axis=0).reshape(N_SEQ * HD, D)
        dinput = jnp.dot(dquery, query_weight[section], preferred_element_type=jnp.float32)
        dinput = dinput + jnp.dot(dkey, wk_rep, preferred_element_type=jnp.float32)
        dinput = dinput + jnp.dot(dvalue, wv_rep, preferred_element_type=jnp.float32)
        grads.append(dinput.astype(jnp.bfloat16))
    grads = grads[1:] + [jnp.zeros_like(grads[0])]
    return jnp.stack(grads, axis=0)
```

```python
import functools
import math

import jax
import jax.numpy as jnp
from jax import lax
from jax.experimental import pallas as pl
from jax.experimental.pallas import tpu as pltpu
from jax.sharding import PartitionSpec as P

HD = 128
CHUNKS = 2


def passed_along(block, axis, distance):
    devices = range(lax.axis_size(axis))
    route = [(i - distance, i) for i in devices if i - distance in devices]
    return lax.ppermute(block, axis, route)


def attend_kernel(start_ref, q_ref, o_ref, k_ref, v_ref, out_ref, dk_acc, dv_acc, *, heads, block):
    head = pl.program_id(0)
    total = k_ref.shape[0]
    scale = 1.0 / math.sqrt(HD)
    nt = (((1,), (1,)), ((), ()))
    tn = (((0,), (0,)), ((), ()))

    @pl.when(head == 0)
    def _():
        dk_acc[...] = jnp.zeros_like(dk_acc)
        dv_acc[...] = jnp.zeros_like(dv_acc)

    for i in range(total // block):
        rows = pl.ds(i * block, block)
        width = (i + 1) * block
        q = q_ref[rows, :]
        o = o_ref[rows, :]
        k = k_ref[pl.ds(0, width), :]
        v = v_ref[pl.ds(0, width), :]
        s = lax.dot_general(k, q, nt, preferred_element_type=jnp.float32)
        key_at = lax.broadcasted_iota(jnp.int32, (width, block), 0)
        query_at = i * block + lax.broadcasted_iota(jnp.int32, (1, block), 1)
        allowed = (key_at <= query_at) & (key_at >= start_ref[:, rows])
        s = jnp.where(allowed, s, -jnp.inf)
        top = jnp.max(s, axis=0, keepdims=True)
        expo = jnp.exp2((s - top) * (scale * math.log2(math.e)))
        prob = expo * (1.0 / jnp.sum(expo, axis=0, keepdims=True))
        dprob = lax.dot_general(v, o, nt, preferred_element_type=jnp.float32)
        delta = jnp.sum(prob * dprob, axis=0, keepdims=True)
        dscore = (prob * ((dprob - delta) * scale)).astype(jnp.bfloat16)
        dq = lax.dot_general(dscore, k, tn, preferred_element_type=jnp.float32)
        out_ref[rows, pl.ds(pl.multiple_of(head * HD, HD), HD)] = dq.astype(jnp.bfloat16)
        dk_acc[pl.ds(0, width), :] += jnp.dot(dscore, q, preferred_element_type=jnp.float32)
        dv_acc[pl.ds(0, width), :] += jnp.dot(
            prob.astype(jnp.bfloat16), o, preferred_element_type=jnp.float32
        )

    @pl.when(head == heads - 1)
    def _():
        out_ref[:, pl.ds(heads * HD, HD)] = dk_acc[...].astype(jnp.bfloat16)
        out_ref[:, pl.ds((heads + 1) * HD, HD)] = dv_acc[...].astype(jnp.bfloat16)


def attend(start, q_all, o_all, k_head, v_head):
    total, width = q_all.shape
    heads = width // HD
    block = min(256, total)
    one_head = pl.BlockSpec((total, HD), lambda h: (0, h))
    shared = pl.BlockSpec((total, HD), lambda h: (0, 0))
    return pl.pallas_call(
        functools.partial(attend_kernel, heads=heads, block=block),
        grid=(heads,),
        in_specs=[pl.BlockSpec((1, total), lambda h: (0, 0)), one_head, one_head, shared, shared],
        out_specs=pl.BlockSpec((total, (heads + 2) * HD), lambda h: (0, 0)),
        out_shape=jax.ShapeDtypeStruct((total, (heads + 2) * HD), jnp.bfloat16),
        scratch_shapes=[pltpu.VMEM((total, HD), jnp.float32), pltpu.VMEM((total, HD), jnp.float32)],
        compiler_params=pltpu.CompilerParams(dimension_semantics=("arbitrary",)),
        name="attend",
    )(start, q_all, o_all, k_head, v_head)


def body(queries, keys, values, out_grad, documents, query_weight, key_weight, value_weight):
    count = lax.axis_size("seq")
    tok = queries.shape[1]
    total = tok * count
    features = query_weight.shape[1]
    kv = keys.shape[2] // HD
    reps = count // kv
    slot_head = lax.axis_index("seq") // reps

    def by_heads(x):
        parts = x.reshape(tok, count, -1).transpose(1, 0, 2)
        got = lax.all_to_all(parts, "seq", split_axis=0, concat_axis=0, tiled=True)
        return got.reshape(total, -1)

    def by_kv_head(x):
        return by_heads(jnp.repeat(x.reshape(tok, kv, HD), reps, axis=1))

    k_head = by_kv_head(keys[0])
    v_head = by_kv_head(values[0])
    q_all = by_heads(queries[0])
    o_all = by_heads(out_grad[0])
    ids = documents[0]
    start = jnp.sum((ids[:, None] < ids[None, :]).astype(jnp.int32), axis=0, keepdims=True)
    grads = attend(start, q_all, o_all, k_head, v_head)

    def rows_of(weight):
        return lax.dynamic_slice_in_dim(weight[0], slot_head * HD, HD, 0)

    weight = jnp.concatenate([query_weight[0], rows_of(key_weight), rows_of(value_weight)], axis=0)
    model = weight.shape[1]
    step = model // CHUNKS
    received = []
    for c in range(CHUNKS):
        part = jnp.dot(
            grads, weight[:, c * step : (c + 1) * step], preferred_element_type=jnp.float32
        ).astype(jnp.bfloat16)
        dinput = lax.psum_scatter(part, "seq", scatter_dimension=0, tiled=True)
        received.append(passed_along(dinput, "section", -1))
    return jnp.concatenate(received, axis=1)[None]


def solution(mesh):
    in_specs = (
        P("section", "seq", None),
        P("section", "seq", None),
        P("section", "seq", None),
        P("section", "seq", None),
        P("section", None),
        P("section", "seq", None),
        P("section", None, None),
        P("section", None, None),
    )
    out_specs = P("section", "seq", None)
    return jax.shard_map(body, mesh=mesh, in_specs=in_specs, out_specs=out_specs, check_vma=False)
```

```python
import functools
import math

import jax
import jax.numpy as jnp
from jax import lax
from jax.experimental import pallas as pl
from jax.experimental.pallas import tpu as pltpu
from jax.sharding import PartitionSpec as P

HD = 128
CHUNKS = 4
CORES = 2


def passed_along(block, axis, distance):
    devices = range(lax.axis_size(axis))
    route = [(i - distance, i) for i in devices if i - distance in devices]
    return lax.ppermute(block, axis, route)


def added(*terms):
    return sum(x.astype(jnp.float32) for x in terms).astype(jnp.bfloat16)


def attend_kernel(start_ref, q_ref, o_ref, k_ref, v_ref, out_ref, dk_acc, dv_acc, *, heads, block):
    head = pl.program_id(0)
    total = k_ref.shape[0]
    scale = 1.0 / math.sqrt(HD)
    nt = (((1,), (1,)), ((), ()))
    tn = (((0,), (0,)), ((), ()))

    @pl.when(head == 0)
    def _():
        dk_acc[...] = jnp.zeros_like(dk_acc)
        dv_acc[...] = jnp.zeros_like(dv_acc)

    for i in range(total // block):
        rows = pl.ds(i * block, block)
        width = (i + 1) * block
        q = q_ref[rows, :]
        o = o_ref[rows, :]
        k = k_ref[pl.ds(0, width), :]
        v = v_ref[pl.ds(0, width), :]
        s = lax.dot_general(k, q, nt, preferred_element_type=jnp.float32)
        key_at = lax.broadcasted_iota(jnp.int32, (width, block), 0)
        query_at = i * block + lax.broadcasted_iota(jnp.int32, (1, block), 1)
        allowed = (key_at <= query_at) & (key_at >= start_ref[:, rows])
        s = jnp.where(allowed, s, -jnp.inf)
        top = jnp.max(s, axis=0, keepdims=True)
        expo = jnp.exp2((s - top) * (scale * math.log2(math.e)))
        prob = expo * (1.0 / jnp.sum(expo, axis=0, keepdims=True))
        dprob = lax.dot_general(v, o, nt, preferred_element_type=jnp.float32)
        delta = jnp.sum(prob * dprob, axis=0, keepdims=True)
        dscore = (prob * ((dprob - delta) * scale)).astype(jnp.bfloat16)
        dq = lax.dot_general(dscore, k, tn, preferred_element_type=jnp.float32)
        out_ref[rows, pl.ds(pl.multiple_of(head * HD, HD), HD)] = dq.astype(jnp.bfloat16)
        dk_acc[pl.ds(0, width), :] += jnp.dot(dscore, q, preferred_element_type=jnp.float32)
        dv_acc[pl.ds(0, width), :] += jnp.dot(
            prob.astype(jnp.bfloat16), o, preferred_element_type=jnp.float32
        )

    @pl.when(head == heads - 1)
    def _():
        out_ref[:, pl.ds(heads * HD, HD)] = dk_acc[...].astype(jnp.bfloat16)
        out_ref[:, pl.ds((heads + 1) * HD, HD)] = dv_acc[...].astype(jnp.bfloat16)


def attend(start, packed):
    total = packed.shape[0]
    heads = packed.shape[1] // HD // 2 - 1
    block = min(256, total)
    slab = (total, HD)
    return pl.pallas_call(
        functools.partial(attend_kernel, heads=heads, block=block),
        grid=(heads,),
        in_specs=[
            pl.BlockSpec((1, total), lambda h: (0, 0)),
            pl.BlockSpec(slab, lambda h: (0, h)),
            pl.BlockSpec(slab, lambda h: (0, heads + h)),
            pl.BlockSpec(slab, lambda h: (0, 2 * heads)),
            pl.BlockSpec(slab, lambda h: (0, 2 * heads + 1)),
        ],
        out_specs=pl.BlockSpec((total, (heads + 2) * HD), lambda h: (0, 0)),
        out_shape=jax.ShapeDtypeStruct((total, (heads + 2) * HD), jnp.bfloat16),
        scratch_shapes=[pltpu.VMEM(slab, jnp.float32), pltpu.VMEM(slab, jnp.float32)],
        compiler_params=pltpu.CompilerParams(dimension_semantics=("arbitrary",)),
        name="attend",
    )(start, packed, packed, packed, packed)


def pack_kernel(q_ref, o_ref, k_ref, v_ref, out_ref):
    width = q_ref.shape[1]
    out_ref[:, pl.ds(0, width)] = q_ref[...]
    out_ref[:, pl.ds(width, width)] = o_ref[...]
    out_ref[:, pl.ds(2 * width, HD)] = k_ref[...]
    out_ref[:, pl.ds(2 * width + HD, HD)] = v_ref[...]


def pack(queries, out_grad, keys, values, count, reps):
    tok = queries.shape[0]
    width = queries.shape[1] // count
    by_slot = pl.BlockSpec((tok, width), lambda j: (0, j))
    by_head = pl.BlockSpec((tok, HD), lambda j: (0, j // reps))
    packed = 2 * (width + HD)
    return pl.pallas_call(
        pack_kernel,
        grid=(count,),
        in_specs=[by_slot, by_slot, by_head, by_head],
        out_specs=pl.BlockSpec((None, tok, packed), lambda j: (j, 0, 0)),
        out_shape=jax.ShapeDtypeStruct((count, tok, packed), queries.dtype),
        compiler_params=pltpu.CompilerParams(dimension_semantics=("arbitrary",)),
        name="pack",
    )(queries, out_grad, keys, values)


def body(queries, keys, values, out_grad, documents, query_weight, key_weight, value_weight):
    count = lax.axis_size("seq")
    tok = queries.shape[1]
    total = tok * count
    kv = keys.shape[2] // HD
    reps = count // kv
    slot_head = lax.axis_index("seq") // reps

    sent = pack(queries[0], out_grad[0], keys[0], values[0], count, reps)
    got = lax.all_to_all(sent, "seq", split_axis=0, concat_axis=0, tiled=True)
    ids = documents[0]
    start = jnp.sum((ids[:, None] < ids[None, :]).astype(jnp.int32), axis=0, keepdims=True)
    grads = attend(start, got.reshape(total, -1))

    def rows_of(weight):
        return lax.dynamic_slice_in_dim(weight[0], slot_head * HD, HD, 0)

    weight = jnp.concatenate([query_weight[0], rows_of(key_weight), rows_of(value_weight)], axis=0)
    model = weight.shape[1]
    step = model // CHUNKS
    chips = count // CORES
    chip = lax.axis_index("seq") // CORES
    core = lax.axis_index("seq") % CORES
    by_core = grads.reshape(chips, CORES, tok, -1)
    mine = lax.dynamic_index_in_dim(by_core, core, 1, False).reshape(chips * tok, -1)
    other = lax.dynamic_index_in_dim(by_core, 1 - core, 1, False).reshape(chips * tok, -1)
    swap = [(i, i ^ 1) for i in range(count)]
    received = []
    for c in range(CHUNKS):
        columns = weight[:, c * step : (c + 1) * step]
        away = jnp.dot(other, columns, preferred_element_type=jnp.float32).astype(jnp.bfloat16)
        away = lax.ppermute(away, "seq", swap)
        here = jnp.dot(mine, columns, preferred_element_type=jnp.float32) + away.astype(jnp.float32)
        here = here.astype(jnp.bfloat16)

        def rows_for(target):
            return lax.dynamic_slice_in_dim(here, target * tok, tok, 0)

        up = down = None
        for r in range(1, chips):
            send_up = rows_for(jnp.minimum(chips - r + chip, chips - 1))
            send_down = rows_for(jnp.maximum(chip + r - chips, 0))
            if r > 1:
                send_up = added(send_up, up)
                send_down = added(send_down, down)
            lower = [i for i in range(count) if i // CORES < r]
            upper = [i for i in range(count) if i // CORES >= chips - r]
            up = lax.ppermute(send_up, "seq", [(i, i + CORES) for i in lower])
            down = lax.ppermute(send_down, "seq", [(i, i - CORES) for i in upper])
        dinput = added(rows_for(chip), up, down)
        received.append(passed_along(dinput, "section", -1))
    return jnp.concatenate(received, axis=1)[None]


def solution(mesh):
    in_specs = (
        P("section", "seq", None),
        P("section", "seq", None),
        P("section", "seq", None),
        P("section", "seq", None),
        P("section", None),
        P("section", "seq", None),
        P("section", None, None),
        P("section", None, None),
    )
    out_specs = P("section", "seq", None)
    return jax.shard_map(body, mesh=mesh, in_specs=in_specs, out_specs=out_specs, check_vma=False)
```

```python
import functools
import math

import jax
import jax.numpy as jnp
from jax import lax
from jax.experimental import pallas as pl
from jax.experimental.pallas import tpu as pltpu
from jax.sharding import PartitionSpec as P

HD = 128
CHUNKS = 4
CORES = 2


def passed_along(block, axis, distance):
    devices = range(lax.axis_size(axis))
    route = [(i - distance, i) for i in devices if i - distance in devices]
    return lax.ppermute(block, axis, route)


def added(*terms):
    return sum(x.astype(jnp.float32) for x in terms).astype(jnp.bfloat16)


def attend_kernel(
    first_ref, start_ref, q_ref, o_ref, k_ref, v_ref, out_ref, dk_acc, dv_acc, *, heads, tok
):
    head = pl.program_id(0)
    total = k_ref.shape[0]
    block = CORES * tok
    blocks = total // block
    half = total // CORES
    scale = 1.0 / math.sqrt(HD)
    nt = (((1,), (1,)), ((), ()))
    tn = (((0,), (0,)), ((), ()))

    @pl.when(head == 0)
    def _():
        dk_acc[...] = jnp.zeros_like(dk_acc)
        dv_acc[...] = jnp.zeros_like(dv_acc)

    def one_block(i, width):
        at = pl.multiple_of(i * block, block)
        low = pl.multiple_of(at + block - width, block)
        rows = pl.ds(at, block)
        window = pl.ds(low, width)
        q = q_ref[rows, :]
        o = o_ref[rows, :]
        k = k_ref[window, :]
        v = v_ref[window, :]
        s = lax.dot_general(k, q, nt, preferred_element_type=jnp.float32)
        key_at = low + lax.broadcasted_iota(jnp.int32, (width, block), 0)
        query_at = at + lax.broadcasted_iota(jnp.int32, (1, block), 1)
        allowed = (key_at <= query_at) & (key_at >= start_ref[:, rows])
        s = jnp.where(allowed, s, -jnp.inf)
        top = jnp.max(s, axis=0, keepdims=True)
        expo = jnp.exp2((s - top) * (scale * math.log2(math.e)))
        prob = expo * (1.0 / jnp.sum(expo, axis=0, keepdims=True))
        dprob = lax.dot_general(v, o, nt, preferred_element_type=jnp.float32)
        delta = jnp.sum(prob * dprob, axis=0, keepdims=True)
        dscore = (prob * ((dprob - delta) * scale)).astype(jnp.bfloat16)
        dq = lax.dot_general(dscore, k, tn, preferred_element_type=jnp.float32)
        columns = pl.ds(pl.multiple_of(head * HD, HD), HD)
        for core in range(CORES):
            to = pl.multiple_of(core * half + i * tok, tok)
            out_ref[pl.ds(to, tok), columns] = dq[core * tok : (core + 1) * tok].astype(jnp.bfloat16)
        dk_acc[window, :] += jnp.dot(dscore, q, preferred_element_type=jnp.float32)
        dv_acc[window, :] += jnp.dot(
            prob.astype(jnp.bfloat16), o, preferred_element_type=jnp.float32
        )

    def step(i, _):
        need = i - first_ref[i] + 1
        for n in range(1, blocks + 1):
            pl.when(need == n)(functools.partial(one_block, i, n * block))
        return 0

    lax.fori_loop(0, blocks, step, 0)

    @pl.when(head == heads - 1)
    def _():
        for device in range(total // tok):
            chip, core = device // CORES, device % CORES
            to = pl.ds(core * half + chip * tok, tok)
            rows = pl.ds(device * tok, tok)
            out_ref[to, pl.ds(heads * HD, HD)] = dk_acc[rows, :].astype(jnp.bfloat16)
            out_ref[to, pl.ds((heads + 1) * HD, HD)] = dv_acc[rows, :].astype(jnp.bfloat16)


def attend(start, packed, tok):
    total = packed.shape[0]
    heads = packed.shape[1] // HD // 2 - 1
    block = CORES * tok
    slab = (total, HD)
    first = start[0, ::block] // block
    return pl.pallas_call(
        functools.partial(attend_kernel, heads=heads, tok=tok),
        grid=(heads,),
        in_specs=[
            pl.BlockSpec(memory_space=pltpu.SMEM),
            pl.BlockSpec((1, total), lambda h: (0, 0)),
            pl.BlockSpec(slab, lambda h: (0, h)),
            pl.BlockSpec(slab, lambda h: (0, heads + h)),
            pl.BlockSpec(slab, lambda h: (0, 2 * heads)),
            pl.BlockSpec(slab, lambda h: (0, 2 * heads + 1)),
        ],
        out_specs=pl.BlockSpec((total, (heads + 2) * HD), lambda h: (0, 0)),
        out_shape=jax.ShapeDtypeStruct((total, (heads + 2) * HD), jnp.bfloat16),
        scratch_shapes=[pltpu.VMEM(slab, jnp.float32), pltpu.VMEM(slab, jnp.float32)],
        compiler_params=pltpu.CompilerParams(dimension_semantics=("arbitrary",)),
        name="attend",
    )(first, start, packed, packed, packed, packed)


def pack_kernel(q_ref, o_ref, k_ref, v_ref, out_ref):
    width = q_ref.shape[1]
    out_ref[:, pl.ds(0, width)] = q_ref[...]
    out_ref[:, pl.ds(width, width)] = o_ref[...]
    out_ref[:, pl.ds(2 * width, HD)] = k_ref[...]
    out_ref[:, pl.ds(2 * width + HD, HD)] = v_ref[...]


def pack(queries, out_grad, keys, values, count, reps):
    tok = queries.shape[0]
    width = queries.shape[1] // count
    by_slot = pl.BlockSpec((tok, width), lambda j: (0, j))
    by_head = pl.BlockSpec((tok, HD), lambda j: (0, j // reps))
    packed = 2 * (width + HD)
    return pl.pallas_call(
        pack_kernel,
        grid=(count,),
        in_specs=[by_slot, by_slot, by_head, by_head],
        out_specs=pl.BlockSpec((None, tok, packed), lambda j: (j, 0, 0)),
        out_shape=jax.ShapeDtypeStruct((count, tok, packed), queries.dtype),
        compiler_params=pltpu.CompilerParams(dimension_semantics=("arbitrary",)),
        name="pack",
    )(queries, out_grad, keys, values)


def body(queries, keys, values, out_grad, documents, query_weight, key_weight, value_weight):
    count = lax.axis_size("seq")
    tok = queries.shape[1]
    total = tok * count
    kv = keys.shape[2] // HD
    reps = count // kv
    slot = lax.axis_index("seq")
    swap = [(i, i ^ 1) for i in range(count)]
    other_weight = lax.ppermute(query_weight[0], "seq", swap)

    sent = pack(queries[0], out_grad[0], keys[0], values[0], count, reps)
    got = lax.all_to_all(sent, "seq", split_axis=0, concat_axis=0, tiled=True)
    ids = documents[0]
    start = jnp.sum((ids[:, None] < ids[None, :]).astype(jnp.int32), axis=0, keepdims=True)
    grads = attend(start, got.reshape(total, -1), tok)

    def weights_of(who, rows):
        def of_head(weight):
            return lax.dynamic_slice_in_dim(weight[0], who // reps * HD, HD, 0)

        return jnp.concatenate([rows, of_head(key_weight), of_head(value_weight)], axis=0)

    weight = weights_of(slot, query_weight[0])
    other_weight = weights_of(slot ^ 1, other_weight)
    model = weight.shape[1]
    step = model // CHUNKS
    chips = count // CORES
    chip = slot // CORES
    core = slot % CORES
    by_core = grads.reshape(CORES, chips * tok, -1)
    mine = lax.dynamic_index_in_dim(by_core, core, 0, False)
    away = lax.ppermute(lax.dynamic_index_in_dim(by_core, 1 - core, 0, False), "seq", swap)
    received = []
    for c in range(CHUNKS):
        columns = slice(c * step, (c + 1) * step)
        here = jnp.dot(mine, weight[:, columns], preferred_element_type=jnp.float32)
        here = here + jnp.dot(away, other_weight[:, columns], preferred_element_type=jnp.float32)
        here = here.astype(jnp.bfloat16)

        def rows_for(target):
            return lax.dynamic_slice_in_dim(here, target * tok, tok, 0)

        up = down = None
        for r in range(1, chips):
            send_up = rows_for(jnp.minimum(chips - r + chip, chips - 1))
            send_down = rows_for(jnp.maximum(chip + r - chips, 0))
            if r > 1:
                send_up = added(send_up, up)
                send_down = added(send_down, down)
            lower = [i for i in range(count) if i // CORES < r]
            upper = [i for i in range(count) if i // CORES >= chips - r]
            up = lax.ppermute(send_up, "seq", [(i, i + CORES) for i in lower])
            down = lax.ppermute(send_down, "seq", [(i, i - CORES) for i in upper])
        dinput = added(rows_for(chip), up, down)
        received.append(passed_along(dinput, "section", -1))
    return jnp.concatenate(received, axis=1)[None]


def solution(mesh):
    in_specs = (
        P("section", "seq", None),
        P("section", "seq", None),
        P("section", "seq", None),
        P("section", "seq", None),
        P("section", None),
        P("section", "seq", None),
        P("section", None, None),
        P("section", None, None),
    )
    out_specs = P("section", "seq", None)
    return jax.shard_map(body, mesh=mesh, in_specs=in_specs, out_specs=out_specs, check_vma=False)
```
